16 devices in a mesh: dp: 2 (over y, z), tp: 8 (over x, core).
Axes of the slice: x: 4, y: 2, z: 1, core: 2. Of those that a mesh axis runs over, the one named last changes fastest.
The devices are a block of a 4x4x8 slice.
Arguments:
- x: bfloat16 [2048, 14336], P(('dp', 'tp')), parts along dimension 0
- gain: bfloat16 [14336], replicated
- wq: bfloat16 [14336, 14336], P(None, 'tp')
- wk: bfloat16 [14336, 14336], P(None, 'tp')
- wv: bfloat16 [14336, 14336], P(None, 'tp')
- wo: bfloat16 [14336, 14336], P('tp')
Outputs:
- output: bfloat16 [2048, 14336], P(('dp', 'tp')), parts along dimension 0
There are 2 independent parts. The reference program is written for one: setup_inputs(seed, part) draws one part's arguments, and reference() takes and returns one part's arrays. A program takes and returns all parts, laid end to end along the dimension named above; an argument that names none is the same for every part.
All inputs are finite; a program needn't handle non-finite values.
Results may differ from the reference program's by a relative error of at most 0.012.
Values are sent between devices in bfloat16 or wider.
A program may use at most 768 MiB of HBM per device.

```python
import jax
import jax.numpy as jnp
from jax import lax

ROWS = 1024
D = 14336
HEADS = 112
KV_HEADS = 112
HEAD = 128
THETA = 10000


def setup_inputs(seed: int = 0, part: int = 0) -> dict:
    kx, kn, kq, kk, kv, ko = jax.random.split(jax.random.key(seed), 6)

    def weights(key, rows, columns):
        return jax.random.normal(key, (rows, columns), jnp.float32) * rows**-0.5

    drawn = {
        "x": jax.random.normal(jax.random.fold_in(kx, part), (ROWS, D), jnp.float32),
        "gain": 1 + 0.1 * jax.random.normal(kn, (D,), jnp.float32),
        "wq": 2 * weights(kq, D, HEADS * HEAD),
        "wk": 2 * weights(kk, D, KV_HEADS * HEAD),
        "wv": 4 * weights(kv, D, KV_HEADS * HEAD),
        "wo": weights(ko, HEADS * HEAD, D),
    }
    return {k: v.astype(jnp.bfloat16) for k, v in drawn.items()}


def normed(x, gain):
    wide = x.astype(jnp.float32)
    scale = lax.rsqrt(jnp.mean(wide * wide, -1, keepdims=True) + 1e-6)
    return (wide * scale * gain.astype(jnp.float32)).astype(jnp.bfloat16)


def turned(t, place, theta):
    half = t.shape[-1] // 2
    angle = place.astype(jnp.float32)[:, None] * theta ** (-jnp.arange(half, dtype=jnp.float32) / half)
    cos, sin = jnp.cos(angle)[:, None], jnp.sin(angle)[:, None]
    a, b = t[..., :half].astype(jnp.float32), t[..., half:].astype(jnp.float32)
    return jnp.concatenate([a * cos - b * sin, b * cos + a * sin], -1).astype(jnp.bfloat16)


def matmul(a, w):
    return jnp.dot(a, w, preferred_element_type=jnp.float32).astype(jnp.bfloat16)


def einsum(form, a, b):
    return jnp.einsum(form, a.astype(jnp.float32), b.astype(jnp.float32))


def attention(q, k, v):
    scores = einsum("tgsd,ugd->gstu", q, k) * q.shape[-1] ** -0.5
    token = jnp.arange(q.shape[0])
    scores = jnp.where(token[:, None] >= token, scores, -jnp.inf)
    weights = jax.nn.softmax(scores, -1).astype(jnp.bfloat16)
    return einsum("gstu,ugd->tgsd", weights, v).astype(jnp.bfloat16)


def reference(x, gain, wq, wk, wv, wo):
    a, place = normed(x, gain), jnp.arange(ROWS)
    q = turned(matmul(a, wq).reshape(ROWS, HEADS, HEAD), place, THETA).reshape(ROWS, KV_HEADS, -1, HEAD)
    k = turned(matmul(a, wk).reshape(ROWS, KV_HEADS, HEAD), place, THETA)
    v = matmul(a, wv).reshape(ROWS, KV_HEADS, HEAD)
    seen = attention(q, k, v).reshape(ROWS, HEADS * HEAD)
    return (x.astype(jnp.float32) + jnp.dot(seen, wo, preferred_element_type=jnp.float32)).astype(jnp.bfloat16)
```

```python
import functools

import jax
import jax.numpy as jnp
import numpy as np
from jax import lax
from jax.experimental import pallas as pl
from jax.experimental.pallas import tpu as pltpu
from jax.sharding import PartitionSpec as P

HEAD = 128
THETA = 10000
LOG2E = 1.4426950408889634
HIDDEN = -2e30
MESH = pl.DeviceIdType.MESH
SETS = (48, 48, 32)
F32, BF16 = jnp.float32, jnp.bfloat16


def _dot(a, b, ca=1, cb=0):
    return lax.dot_general(a, b, (((ca,), (cb,)), ((), ())), preferred_element_type=F32)


def _around(n):
    me = lax.axis_index("tp")
    chips = n // 2
    chip, core = lax.div(me, 2), lax.rem(me, 2)
    at = lambda step: lax.rem(chip + step, chips) * 2 + core
    return me, chip * 2 + 1 - core, at(1), at(chips - 1), at(2)


def _greet(*others):
    barrier = pltpu.get_barrier_semaphore()
    for other in others:
        pl.semaphore_signal(barrier, inc=1, device_id={"tp": other}, device_id_type=MESH)
    pl.semaphore_wait(barrier, len(others))


def _remote(src, dst, send, recv, to):
    return pltpu.make_async_remote_copy(src_ref=src, dst_ref=dst, send_sem=send, recv_sem=recv, device_id={"tp": to}, device_id_type=MESH)


def _ds(k, size):
    return pl.ds(pl.multiple_of(k * size, size), size)


def _turn(t, cos, sin):
    t = t.astype(BF16).astype(F32)
    return (t * cos + pltpu.roll(t, HEAD // 2, 1) * sin).astype(BF16)


KC = 512


def _gather(n, x_ref, gain_ref, cos_ref, sin_ref, wk, wv, xg, ko, vo, xv, acc, wbuf, stage, scale, wsem, ssem, rsem, osem, xsem):
    rows, depth = x_ref.shape
    width = wk.shape[1]
    heads = width // HEAD
    nk = depth // KC
    me, mate, right, left, far = _around(n)

    def weights(k, q):
        return pltpu.make_async_copy((wk, wv)[q].at[_ds(k, KC), :], wbuf.at[lax.rem(k, 2), q], wsem.at[lax.rem(k, 2), q])

    for k in range(2):
        for q in range(2):
            weights(k, q).start()
    _greet(mate, right, left)

    def block(owner, k):
        return xv.at[owner, :, _ds(k, KC)]

    def pass_on(owner, k, kind, to):
        return _remote(block(owner, k), block(owner, k), ssem.at[kind], rsem.at[owner, k], to)

    def arrive(owner, k):
        pass_on(owner, k, 0, mate).wait_recv()

    def squares(k, total):
        wide = x_ref[:, _ds(k, KC)].astype(F32)
        wide = wide * wide
        for i in range(0, KC, 128):
            total += wide[:, i : i + 128]
        return total

    total = lax.fori_loop(0, nk, squares, jnp.zeros((rows, 128), F32))
    scale[...] = jnp.broadcast_to(lax.rsqrt(total.sum(1, keepdims=True) / depth + 1e-6), (rows, 128))

    def own(k):
        wide = x_ref[:, _ds(k, KC)].astype(F32)
        xv[me, :, _ds(k, KC)] = (wide * scale[:, :1] * gain_ref[:, _ds(k, KC)].astype(F32)).astype(BF16)
        for kind, to in ((0, right), (1, left), (2, mate)):
            pass_on(me, k, kind, to).start()

    def sides(k):
        even = lax.rem(k, 2) == 0
        arrive(left, k)
        arrive(right, k)
        pass_on(jnp.where(even, left, right), k, 6, jnp.where(even, right, left)).start()
        pass_on(left, k, 3, mate).start()
        pass_on(right, k, 4, mate).start()

    def opposite(k):
        arrive(far, k)
        pass_on(far, k, 5, mate).start()

    other = lambda t: lax.div(t, 2) * 2 + 1 - lax.rem(t, 2)

    def whole(k):
        for t in (mate, other(right), other(left), other(far)):
            arrive(t, k)

    def out(k):
        return pltpu.make_async_copy(xv.at[:, :, _ds(k, KC)], xg.at[:, :, _ds(k, KC)], xsem)

    own(0)
    own(1)
    sides(0)
    own(2)
    sides(1)
    opposite(0)
    own(3)
    sides(2)
    acc[...] = jnp.zeros_like(acc)
    whole(0)

    def multiply(k, q):
        weights(k, q).wait()
        states = xv[:, :, _ds(k, KC)].reshape(n * rows, KC)
        w = wbuf.at[lax.rem(k, 2), q]
        for i in range(0, width, 256):
            acc[:, q * width + i : q * width + i + 256] += _dot(states, w[:, i : i + 256])

        @pl.when(k + 2 < nk)
        def _():
            weights(k + 2, q).start()

    def chunk(k, carry):
        out(k).start()

        @pl.when(k + 4 < nk)
        def _():
            own(k + 4)

        multiply(k, 0)

        @pl.when(k + 3 < nk)
        def _():
            sides(k + 3)

        @pl.when(k + 1 < nk)
        def _():
            opposite(k + 1)

        multiply(k, 1)

        @pl.when(k + 1 < nk)
        def _():
            whole(k + 1)

        return carry

    lax.fori_loop(0, nk, chunk, 0)

    def store(h, q):
        return pltpu.make_async_copy(stage.at[q, lax.rem(h, 2)], (ko, vo)[q].at[h], osem.at[q, lax.rem(h, 2)])

    def finish(h, carry):
        for q in range(2):
            @pl.when(h >= 2)
            def _():
                store(h - 2, q).wait()

            t = acc[:, pl.ds(pl.multiple_of(q * width + h * HEAD, HEAD), HEAD)]
            stage[q, lax.rem(h, 2)] = _turn(t, cos_ref[...], sin_ref[...]) if q == 0 else t.astype(BF16)
            store(h, q).start()
        return carry

    lax.fori_loop(0, heads, finish, 0)
    for h in (heads - 2, heads - 1):
        for q in range(2):
            store(h, q).wait()
    pltpu.make_async_copy(xv, xg, xsem).wait()
    for kind in range(7):
        _remote(xv.at[me], xv.at[me], ssem.at[kind], rsem.at[me, 0], mate).wait_send()


def gather(n, x, gain, cos, sin, wk, wv):
    rows, depth = x.shape
    width = wk.shape[1]
    heads, tokens = width // HEAD, n * rows
    nk = depth // KC
    vmem, hbm = pl.BlockSpec(memory_space=pltpu.VMEM), pl.BlockSpec(memory_space=pl.ANY)
    flops = 2 * tokens * depth * width * 2
    return pl.pallas_call(
        functools.partial(_gather, n),
        out_shape=[jax.ShapeDtypeStruct((n, rows, depth), BF16)] + [jax.ShapeDtypeStruct((heads, tokens, HEAD), BF16)] * 2,
        in_specs=[vmem] * 4 + [hbm] * 2,
        out_specs=[hbm] * 3,
        scratch_shapes=[
            pltpu.VMEM((n, rows, depth), BF16),
            pltpu.VMEM((tokens, 2 * width), F32),
            pltpu.VMEM((2, 2, KC, width), BF16),
            pltpu.VMEM((2, 2, tokens, HEAD), BF16),
            pltpu.VMEM((rows, 128), F32),
            pltpu.SemaphoreType.DMA((2, 2)),
            pltpu.SemaphoreType.DMA((7,)),
            pltpu.SemaphoreType.DMA((n, nk)),
            pltpu.SemaphoreType.DMA((2, 2)),
            pltpu.SemaphoreType.DMA,
        ],
        compiler_params=pltpu.CompilerParams(collective_id=0, has_side_effects=True, vmem_limit_bytes=63 * 2**20),
        cost_estimate=pl.CostEstimate(flops=flops, bytes_accessed=2 * (2 * depth * width + 2 * tokens * depth), transcendentals=0),
        name="gather",
    )(x, gain, cos, sin, wk, wv)


NC = 1024
KQ = 1792


def _pieces(n, m, rows):
    return [(c, c // m * rows, (min(c + 127, n * m - 1) // m + 1) * rows) for c in range(0, n * m, 128)]


def _finish(n, x, cos_ref, sin_ref, kk, vv, xg, wq, wo, y, qacc, qh, seen, xt, wb, term, half, mates, keep, relay, ends, first, second,
            xres, yres, wsem, tsem, hsem, msem, relay_sem, end_sem, send_sem, xsem, ysem):
    rows, depth = x.shape
    width = wq.shape[1]
    heads = width // HEAD
    nq, nc = depth // KQ, depth // NC
    cuts = [(i, min(NC, width - i)) for i in range(0, width, NC)]
    nu = nq * len(cuts)
    scale = HEAD**-0.5 * LOG2E
    me, mate, right, left, far = _around(n)
    chips = n // 2
    chip, core = lax.div(me, 2), lax.rem(me, 2)
    starts = [sum(SETS[:s]) for s in range(len(SETS))]

    def wq_copy(i, b, slot):
        at, size = cuts[b]
        return pltpu.make_async_copy(wq.at[_ds(i, KQ), at : at + size], wb.at[slot, :, :size], wsem.at[slot])

    def wo_copy(j, slot):
        return pltpu.make_async_copy(wo.at[:, _ds(j, NC)], wb.at[slot], wsem.at[slot])

    q_slot = lambda i, b, s: lax.rem(i * len(cuts) + b + s * (nu + nc), 3)
    o_slot = lambda j, s: lax.rem(j + nu + s * (nu + nc), 3)

    def xt_copy(i, s):
        m = SETS[s]
        return pltpu.make_async_copy(xg.at[:, starts[s] : starts[s] + m, _ds(i, KQ)], xt.at[lax.rem(i, 2), :, :m, :], tsem.at[lax.rem(i, 2)])

    for u in range(2):
        wq_copy(u // len(cuts), u % len(cuts), q_slot(u // len(cuts), u % len(cuts), 0)).start()
    xt_copy(0, 0).start()
    _greet(mate, right, left)

    def to_mate(j, s):
        slot, m = lax.rem(j + s * nc, 4), SETS[s]
        return _remote(half.at[slot, :, :m], mates.at[slot, :, :m], hsem.at[slot], msem.at[slot], mate)

    def sends(j, s):
        m, par, even = SETS[s], s % 2, lax.rem(j, 2) == 0
        cols = _ds(j, NC)
        a = _remote(first.at[0, :m, cols], relay.at[par, :m, cols], send_sem.at[0], relay_sem.at[par, j], jnp.where(even, right, left))
        side = jnp.where(even, 1, 0)
        b = _remote(first.at[1, :m, cols], ends.at[par, side, :m, cols], send_sem.at[1], end_sem.at[par, side, j], jnp.where(even, left, right))
        return a, b

    def last_send(j, s):
        m, par, even = SETS[s], s % 2, lax.rem(j, 2) == 0
        cols = _ds(j, NC)
        side = jnp.where(even, 0, 1)
        return _remote(second.at[:m, cols], ends.at[par, side, :m, cols], send_sem.at[2], end_sem.at[par, side, j], jnp.where(even, right, left))

    def pair_wait(j, s):
        to_mate(j, s).wait_recv()

    def pair_work(j, s):
        slot, m, even = lax.rem(j + s * nc, 4), SETS[s], lax.rem(j, 2) == 0
        cols = _ds(j, NC)
        both = lambda i: term[slot, i, :m] + mates[slot, i, :m].astype(F32)
        near = jnp.where(even, 3, 1)
        keep[0, :m, cols] = both(0)
        keep[1, :m, cols] = both(4 - near)
        first[0, :m, cols] = both(2).astype(BF16)
        first[1, :m, cols] = both(near).astype(BF16)

    def pair_send(j, s):
        for c in sends(j, s):
            c.start()

    def relay_wait(j, s):
        sends(j, s)[0].wait_recv()

    def relay_work(j, s):
        m, cols = SETS[s], _ds(j, NC)
        second[:m, cols] = (keep[1, :m, cols] + relay[s % 2, :m, cols].astype(F32)).astype(BF16)

    def end_wait(j, s):
        sends(j, s)[1].wait_recv()
        last_send(j, s).wait_recv()

    def end_work(j, s):
        m, par, cols = SETS[s], s % 2, _ds(j, NC)
        total = keep[0, :m, cols] + ends[par, 0, :m, cols].astype(F32) + ends[par, 1, :m, cols].astype(F32)
        yres[:m, cols] = (xres[:m, cols].astype(F32) + total).astype(BF16)

    def y_copy(j, s):
        m, cols = SETS[s], _ds(j, NC)
        return pltpu.make_async_copy(yres.at[:m, cols], y.at[starts[s] : starts[s] + m, cols], ysem)

    def x_copy(s):
        m = SETS[s]
        return pltpu.make_async_copy(x.at[starts[s] : starts[s] + m, :], xres.at[:m, :], xsem)

    def sent(s):
        m = SETS[s]
        for kind in range(3):
            _remote(second.at[:m, :], second.at[:m, :], send_sem.at[kind], relay_sem.at[0, 0], mate).wait_send()

    def written(s):
        m = SETS[s]
        pltpu.make_async_copy(yres.at[:m, :], y.at[starts[s] : starts[s] + m, :], ysem).wait()

    def each(lo, hi, work):
        lax.fori_loop(lo, hi, lambda j, c: (work(j), c)[1], 0)

    for s, m in enumerate(SETS):
        size = n * m
        more = s + 1 < len(SETS)

        qacc[:size] = jnp.zeros((size, width), F32)

        def step(i, relayed):
            @pl.when(i + 1 < nq)
            def _():
                xt_copy(i + 1, s).start()

            xt_copy(i, s).wait()
            for b, (at, cut) in enumerate(cuts):
                ahead = b + 2
                i2, b2 = i + ahead // len(cuts), ahead % len(cuts)

                @pl.when(i2 < nq)
                def _():
                    wq_copy(i2, b2, q_slot(i2, b2, s)).start()

                @pl.when(i2 >= nq)
                def _():
                    j2 = (i2 - nq) * len(cuts) + b2
                    wo_copy(j2, o_slot(j2, s)).start()

                slot = q_slot(i, b, s)
                wq_copy(i, b, slot).wait()
                if relayed:
                    relay_wait(i * len(cuts) + b, s - 1)
                    relay_work(i * len(cuts) + b, s - 1)
                states = xt[lax.rem(i, 2), :, :m, :].reshape(size, KQ)
                for o in range(0, cut, 256):
                    qacc[:size, at + o : at + o + 256] += _dot(states, wb[slot, :, o : o + 256])
                if relayed:
                    last_send(i * len(cuts) + b, s - 1).start()

        if s == 0:
            each(0, nq, lambda i: step(i, False))
        else:
            lots = nc // len(cuts)
            each(0, lots, lambda i: step(i, True))
            each(lots, nq, lambda i: step(i, False))
        if more:
            xt_copy(0, s + 1).start()

        cos = cos_ref[:, starts[s] : starts[s] + m, :].reshape(size, HEAD)
        sin = sin_ref[:, starts[s] : starts[s] + m, :].reshape(size, HEAD)

        def turn(h):
            qh[h, :size] = _turn(qacc[:size, _ds(h, HEAD)], cos, sin)

        each(0, heads, turn)

        query = lax.broadcasted_iota(jnp.int32, (1, size), 1)
        owner = sum((query >= b * m).astype(jnp.int32) for b in range(1, n))
        place = owner * (rows - m) + query + starts[s]

        def attend(h):
            ones = jnp.ones((8, n * rows), BF16)
            values = jnp.concatenate([vv[h].T, ones], axis=0)
            found = []
            for at, clear, keys in _pieces(n, m, rows):
                score = _dot(kk[h, :keys], qh[h, at : at + 128], 1, 1)
                key = clear + lax.broadcasted_iota(jnp.int32, (keys - clear, 128), 0)
                tail = jnp.where(key <= place[:, at : at + 128], score[clear:], HIDDEN)
                score = tail if clear == 0 else jnp.concatenate([score[:clear], tail], axis=0)
                top = score.max(axis=0, keepdims=True)
                weight = jnp.exp2((score - top) * scale).astype(BF16)
                mix = _dot(values[:, :keys], weight)
                found.append((mix[:HEAD] * (1 / mix[HEAD : HEAD + 1])).T.astype(BF16))
            found = jnp.concatenate(found, axis=0)
            for t in range(n):
                to = lax.rem(t // 2 - chip + chips, chips) + jnp.where(core == t % 2, 0, chips)
                seen[to, :m, _ds(h, HEAD)] = found[t * m : (t + 1) * m]

        each(0, heads, attend)

        if s > 0:
            sent(s - 1)
            x_copy(s - 1).wait()

        def project(j, paired, ended):
            @pl.when(j + 2 < nc)
            def _():
                wo_copy(j + 2, o_slot(j + 2, s)).start()

            if more:
                @pl.when(j + 2 >= nc)
                def _():
                    u = j + 2 - nc
                    for b in range(len(cuts)):
                        @pl.when(u == b)
                        def _():
                            wq_copy(0, b, q_slot(0, b, s + 1)).start()

            slot = o_slot(j, s)
            if paired:
                pair_wait(j - 2, s)

            @pl.when(j >= 4)
            def _():
                to_mate(j - 4, s).wait_send()

            if ended:
                end_wait(j, s - 1)
            wo_copy(j, slot).wait()
            if paired:
                pair_work(j - 2, s)
            if ended:
                end_work(j, s - 1)
            states = seen[:, :m, :].reshape(size, width)
            ring = lax.rem(j + s * nc, 4)
            for o in range(0, NC, 256):
                got = _dot(states, wb[slot, :, o : o + 256]).reshape(n, m, 256)
                term[ring, :, :m, o : o + 256] = got[:chips]
                half[ring, :, :m, o : o + 256] = got[chips:].astype(BF16)
            to_mate(j, s).start()
            if paired:
                pair_send(j - 2, s)
            if ended:
                y_copy(j, s - 1).start()

        each(0, 2, lambda j: project(j, False, s > 0))
        each(2, nc, lambda j: project(j, True, s > 0))
        for j in (nc - 2, nc - 1):
            pair_wait(j, s)
            pair_work(j, s)
            pair_send(j, s)
        for j in range(nc - 4, nc):
            to_mate(j, s).wait_send()
        if s > 0:
            written(s - 1)
        x_copy(s).start()

    last = len(SETS) - 1
    x_copy(last).wait()

    def relay_all(j):
        relay_wait(j, last)
        relay_work(j, last)
        last_send(j, last).start()

    def end_all(j):
        end_wait(j, last)
        end_work(j, last)
        y_copy(j, last).start()

    each(0, nc, relay_all)
    each(0, nc, end_all)
    sent(last)
    written(last)


def finish(n, x, cos, sin, kk, vv, xg, wq, wo):
    rows, depth = x.shape
    width = wq.shape[1]
    heads, tokens = width // HEAD, n * rows
    nc, chips, m = depth // NC, n // 2, max(SETS)
    vmem, hbm = pl.BlockSpec(memory_space=pltpu.VMEM), pl.BlockSpec(memory_space=pl.ANY)
    flops = 2 * tokens * depth * width * 2
    dma = pltpu.SemaphoreType.DMA
    return pl.pallas_call(
        functools.partial(_finish, n),
        out_shape=jax.ShapeDtypeStruct((rows, depth), BF16),
        in_specs=[hbm, vmem, vmem, vmem, vmem, hbm, hbm, hbm],
        out_specs=hbm,
        scratch_shapes=[
            pltpu.VMEM((n * m, width), F32),
            pltpu.VMEM((heads, n * m, HEAD), BF16),
            pltpu.VMEM((n, m, width), BF16),
            pltpu.VMEM((2, n, m, KQ), BF16),
            pltpu.VMEM((3, KQ, NC), BF16),
            pltpu.VMEM((4, chips, m, NC), F32),
            pltpu.VMEM((4, chips, m, NC), BF16),
            pltpu.VMEM((4, chips, m, NC), BF16),
            pltpu.VMEM((2, m, depth), F32),
            pltpu.VMEM((2, m, depth), BF16),
            pltpu.VMEM((2, 2, m, depth), BF16),
            pltpu.VMEM((2, m, depth), BF16),
            pltpu.VMEM((m, depth), BF16),
            pltpu.VMEM((m, depth), BF16),
            pltpu.VMEM((m, depth), BF16),
            dma((3,)), dma((2,)), dma((4,)), dma((4,)), dma((2, nc)), dma((2, 2, nc)), dma((3,)), dma, dma,
        ],
        compiler_params=pltpu.CompilerParams(collective_id=1, has_side_effects=True, vmem_limit_bytes=63 * 2**20),
        cost_estimate=pl.CostEstimate(flops=flops, bytes_accessed=2 * 2 * 3 * depth * width, transcendentals=0),
        name="finish",
    )(x, cos, sin, kk, vv, xg, wq, wo)


def solution(mesh):
    n = mesh.shape["tp"]

    def step(x, gain, wq, wk, wv, wo):
        rows = x.shape[0]
        half = HEAD // 2
        angle = np.arange(n * rows)[:, None] * float(THETA) ** (-np.arange(half) / half)
        cos = np.concatenate([np.cos(angle), np.cos(angle)], 1).astype(np.float32)
        sin = np.concatenate([-np.sin(angle), np.sin(angle)], 1).astype(np.float32)
        xg, kk, vv = gather(n, x, gain[None], jnp.asarray(cos), jnp.asarray(sin), wk, wv)
        shape = (n, rows, HEAD)
        return finish(n, x, jnp.asarray(cos).reshape(shape), jnp.asarray(sin).reshape(shape), kk, vv, xg, wq, wo)

    tokens, columns = P(("dp", "tp"), None), P(None, "tp")
    return jax.shard_map(
        step,
        mesh=mesh,
        in_specs=(tokens, P(None), columns, columns, columns, P("tp", None)),
        out_specs=tokens,
        check_vma=False,
    )
```

```python
import functools

import jax
import jax.numpy as jnp
import numpy as np
from jax import lax
from jax.experimental import pallas as pl
from jax.experimental.pallas import tpu as pltpu
from jax.sharding import PartitionSpec as P

HEAD = 128
THETA = 10000
LOG2E = 1.4426950408889634
MESH = pl.DeviceIdType.MESH
SETS = (48, 48, 32)
F32, BF16 = jnp.float32, jnp.bfloat16


def _dot(a, b, ca=1, cb=0):
    return lax.dot_general(a, b, (((ca,), (cb,)), ((), ())), preferred_element_type=F32)


def _around(n):
    me = lax.axis_index("tp")
    chips = n // 2
    chip, core = lax.div(me, 2), lax.rem(me, 2)
    at = lambda step: lax.rem(chip + step, chips) * 2 + core
    return me, chip * 2 + 1 - core, at(1), at(chips - 1), at(2)


def _greet(*others):
    barrier = pltpu.get_barrier_semaphore()
    for other in others:
        pl.semaphore_signal(barrier, inc=1, device_id={"tp": other}, device_id_type=MESH)
    pl.semaphore_wait(barrier, len(others))


def _remote(src, dst, send, recv, to):
    return pltpu.make_async_remote_copy(src_ref=src, dst_ref=dst, send_sem=send, recv_sem=recv, device_id={"tp": to}, device_id_type=MESH)


def _ds(k, size):
    return pl.ds(pl.multiple_of(k * size, size), size)


def _turn(t, cos, sin):
    t = t.astype(BF16).astype(F32)
    return (t * cos + pltpu.roll(t, HEAD // 2, 1) * sin).astype(BF16)


KC = 512


def _gather(n, x_ref, gain_ref, cos_ref, sin_ref, wk, wv, xg, ko, vo, xv, acc, wbuf, stage, scale, wsem, ssem, rsem, osem, xsem):
    rows, depth = x_ref.shape
    width = wk.shape[1]
    heads = width // HEAD
    nk = depth // KC
    me, mate, right, left, far = _around(n)

    def weights(k, q):
        return pltpu.make_async_copy((wk, wv)[q].at[_ds(k, KC), :], wbuf.at[lax.rem(k, 2), q], wsem.at[lax.rem(k, 2), q])

    for k in range(2):
        for q in range(2):
            weights(k, q).start()
    _greet(mate, right, left)

    def block(owner, k):
        return xv.at[owner, :, _ds(k, KC)]

    def pass_on(owner, k, kind, to):
        return _remote(block(owner, k), block(owner, k), ssem.at[kind], rsem.at[owner, k], to)

    def arrive(owner, k):
        pass_on(owner, k, 0, mate).wait_recv()

    def squares(k, total):
        wide = x_ref[:, _ds(k, KC)].astype(F32)
        wide = wide * wide
        for i in range(0, KC, 128):
            total += wide[:, i : i + 128]
        return total

    total = lax.fori_loop(0, nk, squares, jnp.zeros((rows, 128), F32))
    scale[...] = jnp.broadcast_to(lax.rsqrt(total.sum(1, keepdims=True) / depth + 1e-6), (rows, 128))

    def norm(k):
        wide = x_ref[:, _ds(k, KC)].astype(F32)
        xv[me, :, _ds(k, KC)] = (wide * scale[:, :1] * gain_ref[:, _ds(k, KC)].astype(F32)).astype(BF16)

    def own(k):
        for kind, to in ((0, right), (1, left), (2, mate)):
            pass_on(me, k, kind, to).start()

    def sides(k):
        even = lax.rem(k, 2) == 0
        arrive(left, k)
        arrive(right, k)
        pass_on(jnp.where(even, left, right), k, 6, jnp.where(even, right, left)).start()
        pass_on(left, k, 3, mate).start()
        pass_on(right, k, 4, mate).start()

    def opposite(k):
        arrive(far, k)
        pass_on(far, k, 5, mate).start()

    other = lambda t: lax.div(t, 2) * 2 + 1 - lax.rem(t, 2)

    def whole(k):
        for t in (mate, other(right), other(left), other(far)):
            arrive(t, k)

    def out(k):
        return pltpu.make_async_copy(xv.at[:, :, _ds(k, KC)], xg.at[:, :, _ds(k, KC)], xsem)

    for k in range(2):
        norm(k)
        own(k)
    lax.fori_loop(2, nk, lambda k, c: (norm(k), c)[1], 0)
    sides(0)
    own(2)
    sides(1)
    opposite(0)
    own(3)
    sides(2)
    acc[...] = jnp.zeros_like(acc)
    whole(0)

    def product(k, q, i):
        states = xv[:, :, _ds(k, KC)].reshape(n * rows, KC)
        return acc[:, q * width + i : q * width + i + 256] + _dot(states, wbuf[lax.rem(k, 2), q, :, i : i + 256])

    def multiply(k, q):
        weights(k, q).wait()
        for i in range(0, width, 256):
            acc[:, q * width + i : q * width + i + 256] = product(k, q, i)

        @pl.when(k + 2 < nk)
        def _():
            weights(k + 2, q).start()

    def chunk(k, carry):
        out(k).start()

        @pl.when(k + 4 < nk)
        def _():
            own(k + 4)

        multiply(k, 0)

        @pl.when(k + 3 < nk)
        def _():
            sides(k + 3)

        opposite(k + 1)
        multiply(k, 1)
        whole(k + 1)
        return carry

    lax.fori_loop(0, nk - 1, chunk, 0)

    def store(h, q):
        return pltpu.make_async_copy(stage.at[q, h % 4], (ko, vo)[q].at[h], osem.at[q, h % 4])

    out(nk - 1).start()
    for q in range(2):
        weights(nk - 1, q).wait()
        for i in range(0, width, 256):
            total = product(nk - 1, q, i)
            for h in (i // HEAD, i // HEAD + 1):
                if h >= 4:
                    store(h - 4, q).wait()
                t = total[:, h * HEAD - i : (h + 1) * HEAD - i]
                stage[q, h % 4] = _turn(t, cos_ref[...], sin_ref[...]) if q == 0 else t.astype(BF16)
                store(h, q).start()
    for q in range(2):
        for h in range(heads - 4, heads):
            store(h, q).wait()
    pltpu.make_async_copy(xv, xg, xsem).wait()
    for kind in range(7):
        _remote(xv.at[me], xv.at[me], ssem.at[kind], rsem.at[me, 0], mate).wait_send()


def gather(n, x, gain, cos, sin, wk, wv):
    rows, depth = x.shape
    width = wk.shape[1]
    heads, tokens = width // HEAD, n * rows
    nk = depth // KC
    vmem, hbm = pl.BlockSpec(memory_space=pltpu.VMEM), pl.BlockSpec(memory_space=pl.ANY)
    flops = 2 * tokens * depth * width * 2
    return pl.pallas_call(
        functools.partial(_gather, n),
        out_shape=[jax.ShapeDtypeStruct((n, rows, depth), BF16)] + [jax.ShapeDtypeStruct((heads, tokens, HEAD), BF16)] * 2,
        in_specs=[vmem] * 4 + [hbm] * 2,
        out_specs=[hbm] * 3,
        scratch_shapes=[
            pltpu.VMEM((n, rows, depth), BF16),
            pltpu.VMEM((tokens, 2 * width), F32),
            pltpu.VMEM((2, 2, KC, width), BF16),
            pltpu.VMEM((2, 4, tokens, HEAD), BF16),
            pltpu.VMEM((rows, 128), F32),
            pltpu.SemaphoreType.DMA((2, 2)),
            pltpu.SemaphoreType.DMA((7,)),
            pltpu.SemaphoreType.DMA((n, nk)),
            pltpu.SemaphoreType.DMA((2, 4)),
            pltpu.SemaphoreType.DMA,
        ],
        compiler_params=pltpu.CompilerParams(collective_id=0, has_side_effects=True, vmem_limit_bytes=63 * 2**20),
        cost_estimate=pl.CostEstimate(flops=flops, bytes_accessed=2 * (2 * depth * width + 2 * tokens * depth), transcendentals=0),
        name="gather",
    )(x, gain, cos, sin, wk, wv)


NC = 1024
KQ = 1792


def _finish(n, x, cos_ref, sin_ref, kh, vh, xg, wq, wo, y, qacc, qh, seen, xt, wb, term, half, mates, keep, relay, ends, first, second,
            xres, yres, kk, vv, cap, wsem, tsem, hsem, msem, relay_sem, end_sem, send_sem, xsem, ysem, ksem):
    rows, depth = x.shape
    width = wq.shape[1]
    heads = width // HEAD
    nq, nc = depth // KQ, depth // NC
    cuts = [(i, min(NC, width - i)) for i in range(0, width, NC)]
    nu = nq * len(cuts)
    scale = HEAD**-0.5 * LOG2E
    me, mate, right, left, far = _around(n)
    chips = n // 2
    chip, core = lax.div(me, 2), lax.rem(me, 2)
    starts = [sum(SETS[:s]) for s in range(len(SETS))]

    def wq_copy(i, b, slot):
        at, size = cuts[b]
        return pltpu.make_async_copy(wq.at[_ds(i, KQ), at : at + size], wb.at[slot, :, :size], wsem.at[slot])

    def wo_copy(j, slot):
        return pltpu.make_async_copy(wo.at[:, _ds(j, NC)], wb.at[slot], wsem.at[slot])

    q_slot = lambda i, b, s: lax.rem(i * len(cuts) + b + s * (nu + nc), 3)
    o_slot = lambda j, s: lax.rem(j + nu + s * (nu + nc), 3)

    def xt_copy(i, s):
        m = SETS[s]
        return pltpu.make_async_copy(xg.at[:, starts[s] : starts[s] + m, _ds(i, KQ)], xt.at[lax.rem(i, 2), :, :m, :], tsem.at[lax.rem(i, 2)])

    for u in range(2):
        wq_copy(u // len(cuts), u % len(cuts), q_slot(u // len(cuts), u % len(cuts), 0)).start()
    xt_copy(0, 0).start()
    kv_copies = [pltpu.make_async_copy(a, b, ksem.at[i]) for i, (a, b) in enumerate(((kh, kk), (vh, vv)))]
    for c in kv_copies:
        c.start()
    _greet(mate, right, left)

    def to_mate(j, s):
        slot, m = lax.rem(j + s * nc, 4), SETS[s]
        return _remote(half.at[slot, :, :m], mates.at[slot, :, :m], hsem.at[slot], msem.at[slot], mate)

    def sends(j, s):
        m, par, even = SETS[s], s % 2, lax.rem(j, 2) == 0
        cols = _ds(j, NC)
        a = _remote(first.at[0, :m, cols], relay.at[par, :m, cols], send_sem.at[0], relay_sem.at[par, j], jnp.where(even, right, left))
        side = jnp.where(even, 1, 0)
        b = _remote(first.at[1, :m, cols], ends.at[par, side, :m, cols], send_sem.at[1], end_sem.at[par, side, j], jnp.where(even, left, right))
        return a, b

    def last_send(j, s):
        m, par, even = SETS[s], s % 2, lax.rem(j, 2) == 0
        cols = _ds(j, NC)
        side = jnp.where(even, 0, 1)
        return _remote(second.at[:m, cols], ends.at[par, side, :m, cols], send_sem.at[2], end_sem.at[par, side, j], jnp.where(even, right, left))

    def pair_wait(j, s):
        to_mate(j, s).wait_recv()

    def pair_work(j, s):
        slot, m, even = lax.rem(j + s * nc, 4), SETS[s], lax.rem(j, 2) == 0
        cols = _ds(j, NC)
        both = lambda i: term[slot, i, :m] + mates[slot, i, :m].astype(F32)
        near = jnp.where(even, 3, 1)
        keep[0, :m, cols] = both(0)
        keep[1, :m, cols] = both(4 - near)
        first[0, :m, cols] = both(2).astype(BF16)
        first[1, :m, cols] = both(near).astype(BF16)

    def pair_send(j, s):
        for c in sends(j, s):
            c.start()

    def relay_wait(j, s):
        sends(j, s)[0].wait_recv()

    def relay_work(j, s):
        m, cols = SETS[s], _ds(j, NC)
        second[:m, cols] = (keep[1, :m, cols] + relay[s % 2, :m, cols].astype(F32)).astype(BF16)

    def end_wait(j, s):
        sends(j, s)[1].wait_recv()
        last_send(j, s).wait_recv()

    def end_work(j, s):
        m, par, cols = SETS[s], s % 2, _ds(j, NC)
        total = keep[0, :m, cols] + ends[par, 0, :m, cols].astype(F32) + ends[par, 1, :m, cols].astype(F32)
        yres[:m, cols] = (xres[:m, cols].astype(F32) + total).astype(BF16)

    def y_copy(j, s):
        m, cols = SETS[s], _ds(j, NC)
        return pltpu.make_async_copy(yres.at[:m, cols], y.at[starts[s] : starts[s] + m, cols], ysem)

    def x_copy(s):
        m = SETS[s]
        return pltpu.make_async_copy(x.at[starts[s] : starts[s] + m, :], xres.at[:m, :], xsem)

    def sent(s):
        m = SETS[s]
        for kind in range(3):
            _remote(second.at[:m, :], second.at[:m, :], send_sem.at[kind], relay_sem.at[0, 0], mate).wait_send()

    def written(s):
        m = SETS[s]
        pltpu.make_async_copy(yres.at[:m, :], y.at[starts[s] : starts[s] + m, :], ysem).wait()

    def each(lo, hi, work):
        lax.fori_loop(lo, hi, lambda j, c: (work(j), c)[1], 0)

    for s, m in enumerate(SETS):
        size = n * m
        more = s + 1 < len(SETS)

        qacc[:size] = jnp.zeros((size, width), F32)

        def step(i, relayed):
            @pl.when(i + 1 < nq)
            def _():
                xt_copy(i + 1, s).start()

            xt_copy(i, s).wait()
            for b, (at, cut) in enumerate(cuts):
                ahead = b + 2
                i2, b2 = i + ahead // len(cuts), ahead % len(cuts)

                @pl.when(i2 < nq)
                def _():
                    wq_copy(i2, b2, q_slot(i2, b2, s)).start()

                @pl.when(i2 >= nq)
                def _():
                    j2 = (i2 - nq) * len(cuts) + b2
                    wo_copy(j2, o_slot(j2, s)).start()

                slot = q_slot(i, b, s)
                wq_copy(i, b, slot).wait()
                if relayed:
                    relay_wait(i * len(cuts) + b, s - 1)
                    relay_work(i * len(cuts) + b, s - 1)
                states = xt[lax.rem(i, 2), :, :m, :].reshape(size, KQ)
                for o in range(0, cut, 256):
                    qacc[:size, at + o : at + o + 256] += _dot(states, wb[slot, :, o : o + 256])
                if relayed:
                    last_send(i * len(cuts) + b, s - 1).start()

        if s == 0:
            each(0, nq, lambda i: step(i, False))
        else:
            lots = nc // len(cuts)
            each(0, lots, lambda i: step(i, True))
            each(lots, nq, lambda i: step(i, False))
        if more:
            xt_copy(0, s + 1).start()

        cos = cos_ref[:, starts[s] : starts[s] + m, :].reshape(size, HEAD)
        sin = sin_ref[:, starts[s] : starts[s] + m, :].reshape(size, HEAD)

        def turn(h):
            qh[h, :size] = _turn(qacc[:size, _ds(h, HEAD)], cos, sin)

        each(0, heads, turn)

        if s == 0:
            for c in kv_copies:
                c.wait()
        band, keys = 2 * m, 2 * rows
        row, key = (lax.broadcasted_iota(jnp.int32, (band, keys), i) for i in range(2))
        cap[:band] = jnp.where(key <= row + starts[s] + jnp.where(row < m, 0, rows - m), jnp.inf, -jnp.inf)

        def attend(h):
            bands = range(chips)
            cut = lambda a, i, size=band: a[i * size : (i + 1) * size]
            scores = [_dot(qh[h, b * band : size], kk[h, b * keys : (b + 1) * keys], 1, 1) for b in bands]
            weights = []
            for g in bands:
                mine = [cut(scores[b], g - b) for b in range(g + 1)]
                mine[g] = jnp.minimum(mine[g], cap[:band])
                top = functools.reduce(jnp.maximum, mine).max(axis=1, keepdims=True)
                weights.append([jnp.exp2((score - top) * scale).astype(BF16) for score in mine])
            ones = jnp.ones((keys, HEAD), BF16)
            mixes = []
            for b in bands:
                values = jnp.concatenate([vv[h, b * keys : (b + 1) * keys], ones], axis=1)
                mixes.append(_dot(jnp.concatenate([weights[g][b] for g in range(b, chips)], axis=0), values))
            for g in bands:
                mix = sum(cut(mixes[b], g - b) for b in range(g + 1))
                found = (mix[:, :HEAD] / mix[:, HEAD:]).astype(BF16)
                for i in range(2):
                    to = lax.rem(g - chip + chips, chips) + jnp.where(core == i, 0, chips)
                    seen[to, :m, _ds(h, HEAD)] = cut(found, i, m)

        each(0, heads, attend)

        if s > 0:
            sent(s - 1)
            x_copy(s - 1).wait()

        def project(j, paired, ended):
            @pl.when(j + 2 < nc)
            def _():
                wo_copy(j + 2, o_slot(j + 2, s)).start()

            if more:
                @pl.when(j + 2 >= nc)
                def _():
                    u = j + 2 - nc
                    for b in range(len(cuts)):
                        @pl.when(u == b)
                        def _():
                            wq_copy(0, b, q_slot(0, b, s + 1)).start()

            slot = o_slot(j, s)
            if paired:
                pair_wait(j - 2, s)

            @pl.when(j >= 4)
            def _():
                to_mate(j - 4, s).wait_send()

            if ended:
                end_wait(j, s - 1)
            wo_copy(j, slot).wait()
            if paired:
                pair_work(j - 2, s)
            if ended:
                end_work(j, s - 1)
            states = seen[:, :m, :].reshape(size, width)
            ring = lax.rem(j + s * nc, 4)
            for o in range(0, NC, 256):
                got = _dot(states, wb[slot, :, o : o + 256]).reshape(n, m, 256)
                term[ring, :, :m, o : o + 256] = got[:chips]
                half[ring, :, :m, o : o + 256] = got[chips:].astype(BF16)
            to_mate(j, s).start()
            if paired:
                pair_send(j - 2, s)
            if ended:
                y_copy(j, s - 1).start()

        each(0, 2, lambda j: project(j, False, s > 0))
        each(2, nc, lambda j: project(j, True, s > 0))
        for j in (nc - 2, nc - 1):
            pair_wait(j, s)
            pair_work(j, s)
            pair_send(j, s)
        for j in range(nc - 4, nc):
            to_mate(j, s).wait_send()
        if s > 0:
            written(s - 1)
        x_copy(s).start()

    last = len(SETS) - 1
    x_copy(last).wait()

    def relay_all(j):
        relay_wait(j, last)
        relay_work(j, last)
        last_send(j, last).start()

    def end_all(j):
        end_wait(j, last)
        end_work(j, last)
        y_copy(j, last).start()

    each(0, nc, relay_all)
    each(0, nc, end_all)
    sent(last)
    written(last)


def finish(n, x, cos, sin, kk, vv, xg, wq, wo):
    rows, depth = x.shape
    width = wq.shape[1]
    heads, tokens = width // HEAD, n * rows
    nc, chips, m = depth // NC, n // 2, max(SETS)
    vmem, hbm = pl.BlockSpec(memory_space=pltpu.VMEM), pl.BlockSpec(memory_space=pl.ANY)
    flops = 2 * tokens * depth * width * 2
    dma = pltpu.SemaphoreType.DMA
    return pl.pallas_call(
        functools.partial(_finish, n),
        out_shape=jax.ShapeDtypeStruct((rows, depth), BF16),
        in_specs=[hbm, vmem, vmem, hbm, hbm, hbm, hbm, hbm],
        out_specs=hbm,
        scratch_shapes=[
            pltpu.VMEM((n * m, width), F32),
            pltpu.VMEM((heads, n * m, HEAD), BF16),
            pltpu.VMEM((n, m, width), BF16),
            pltpu.VMEM((2, n, m, KQ), BF16),
            pltpu.VMEM((3, KQ, NC), BF16),
            pltpu.VMEM((4, chips, m, NC), F32),
            pltpu.VMEM((4, chips, m, NC), BF16),
            pltpu.VMEM((4, chips, m, NC), BF16),
            pltpu.VMEM((2, m, depth), F32),
            pltpu.VMEM((2, m, depth), BF16),
            pltpu.VMEM((2, 2, m, depth), BF16),
            pltpu.VMEM((2, m, depth), BF16),
            pltpu.VMEM((m, depth), BF16),
            pltpu.VMEM((m, depth), BF16),
            pltpu.VMEM((m, depth), BF16),
            pltpu.VMEM((heads, tokens, HEAD), BF16),
            pltpu.VMEM((heads, tokens, HEAD), BF16),
            pltpu.VMEM((2 * m, 2 * rows), F32),
            dma((3,)), dma((2,)), dma((4,)), dma((4,)), dma((2, nc)), dma((2, 2, nc)), dma((3,)), dma, dma, dma((2,)),
        ],
        compiler_params=pltpu.CompilerParams(collective_id=1, has_side_effects=True, vmem_limit_bytes=63 * 2**20),
        cost_estimate=pl.CostEstimate(flops=flops, bytes_accessed=2 * 2 * 3 * depth * width, transcendentals=0),
        name="finish",
    )(x, cos, sin, kk, vv, xg, wq, wo)


def solution(mesh):
    n = mesh.shape["tp"]

    def step(x, gain, wq, wk, wv, wo):
        rows = x.shape[0]
        half = HEAD // 2
        angle = np.arange(n * rows)[:, None] * float(THETA) ** (-np.arange(half) / half)
        cos = np.concatenate([np.cos(angle), np.cos(angle)], 1).astype(np.float32)
        sin = np.concatenate([-np.sin(angle), np.sin(angle)], 1).astype(np.float32)
        xg, kk, vv = gather(n, x, gain[None], jnp.asarray(cos), jnp.asarray(sin), wk, wv)
        shape = (n, rows, HEAD)
        return finish(n, x, jnp.asarray(cos).reshape(shape), jnp.asarray(sin).reshape(shape), kk, vv, xg, wq, wo)

    tokens, columns = P(("dp", "tp"), None), P(None, "tp")
    return jax.shard_map(
        step,
        mesh=mesh,
        in_specs=(tokens, P(None), columns, columns, columns, P("tp", None)),
        out_specs=tokens,
        check_vma=False,
    )
```

```python
import functools

import jax
import jax.numpy as jnp
import numpy as np
from jax import lax
from jax.experimental import pallas as pl
from jax.experimental.pallas import tpu as pltpu
from jax.sharding import PartitionSpec as P

HEAD = 128
THETA = 10000
LOG2E = 1.4426950408889634
MESH = pl.DeviceIdType.MESH
SETS = (48, 48, 32)
F32, BF16 = jnp.float32, jnp.bfloat16
PAD = 128


def _dot(a, b, ca=1, cb=0):
    return lax.dot_general(a, b, (((ca,), (cb,)), ((), ())), preferred_element_type=F32)


def _around(n):
    me = lax.axis_index("tp")
    chips = n // 2
    chip, core = lax.div(me, 2), lax.rem(me, 2)
    at = lambda step: lax.rem(chip + step, chips) * 2 + core
    return me, chip * 2 + 1 - core, at(1), at(chips - 1), at(2)


def _greet(*others):
    barrier = pltpu.get_barrier_semaphore()
    for other in others:
        pl.semaphore_signal(barrier, inc=1, device_id={"tp": other}, device_id_type=MESH)
    pl.semaphore_wait(barrier, len(others))


def _remote(src, dst, send, recv, to):
    return pltpu.make_async_remote_copy(src_ref=src, dst_ref=dst, send_sem=send, recv_sem=recv, device_id={"tp": to}, device_id_type=MESH)


def _ds(k, size):
    return pl.ds(pl.multiple_of(k * size, size), size)


def _turn(t, cos, sin):
    t = t.astype(BF16).astype(F32)
    return (t * cos + pltpu.roll(t, HEAD // 2, 1) * sin).astype(BF16)


KC = 512


def _gather(n, x_ref, gain_ref, cos_ref, sin_ref, wk, wv, xg, ko, vo, xv, acc, wbuf, stage, scale, wsem, ssem, rsem, osem, xsem):
    rows, depth = x_ref.shape
    width = wk.shape[1]
    heads = width // HEAD
    nk = depth // KC
    me, mate, right, left, far = _around(n)

    def weights(k, q):
        return pltpu.make_async_copy((wk, wv)[q].at[_ds(k, KC), :], wbuf.at[lax.rem(k, 2), q], wsem.at[lax.rem(k, 2), q])

    for k in range(2):
        for q in range(2):
            weights(k, q).start()
    _greet(mate, right, left)

    def block(owner, k):
        return xv.at[owner, :, _ds(k, KC)]

    def pass_on(owner, k, kind, to):
        return _remote(block(owner, k), block(owner, k), ssem.at[kind], rsem.at[owner, k], to)

    def arrive(owner, k):
        pass_on(owner, k, 0, mate).wait_recv()

    def squares(k, total):
        wide = x_ref[:, _ds(k, KC)].astype(F32)
        wide = wide * wide
        for i in range(0, KC, 128):
            total += wide[:, i : i + 128]
        return total

    total = lax.fori_loop(0, nk, squares, jnp.zeros((rows, 128), F32))
    scale[...] = jnp.broadcast_to(lax.rsqrt(total.sum(1, keepdims=True) / depth + 1e-6), (rows, 128))

    def norm(k):
        wide = x_ref[:, _ds(k, KC)].astype(F32)
        xv[me, :, _ds(k, KC)] = (wide * scale[:, :1] * gain_ref[:, _ds(k, KC)].astype(F32)).astype(BF16)

    def own(k):
        for kind, to in ((0, right), (1, left), (2, mate)):
            pass_on(me, k, kind, to).start()

    def sides(k):
        even = lax.rem(k, 2) == 0
        arrive(left, k)
        arrive(right, k)
        pass_on(jnp.where(even, left, right), k, 6, jnp.where(even, right, left)).start()
        pass_on(left, k, 3, mate).start()
        pass_on(right, k, 4, mate).start()

    def opposite(k):
        arrive(far, k)
        pass_on(far, k, 5, mate).start()

    other = lambda t: lax.div(t, 2) * 2 + 1 - lax.rem(t, 2)

    def whole(k):
        for t in (mate, other(right), other(left), other(far)):
            arrive(t, k)

    def out(k):
        return pltpu.make_async_copy(xv.at[:, :, _ds(k, KC)], xg.at[:, :, _ds(k, KC)], xsem)

    for k in range(2):
        norm(k)
        own(k)
    lax.fori_loop(2, nk, lambda k, c: (norm(k), c)[1], 0)
    sides(0)
    own(2)
    sides(1)
    opposite(0)
    own(3)
    sides(2)
    acc[...] = jnp.zeros_like(acc)
    whole(0)

    def product(k, q, i):
        states = xv[:, :, _ds(k, KC)].reshape(n * rows, KC)
        return acc[q, :, i : i + 256] + _dot(states, wbuf[lax.rem(k, 2), q, :, i : i + 256])

    def multiply(k, q):
        weights(k, q).wait()
        for i in range(0, width, 256):
            acc[q, :, i : i + 256] = product(k, q, i)

        @pl.when(k + 2 < nk)
        def _():
            weights(k + 2, q).start()

    def chunk(k, carry):
        out(k).start()

        @pl.when(k + 4 < nk)
        def _():
            own(k + 4)

        multiply(k, 0)

        @pl.when(k + 3 < nk)
        def _():
            sides(k + 3)

        opposite(k + 1)
        multiply(k, 1)
        whole(k + 1)
        return carry

    lax.fori_loop(0, nk - 1, chunk, 0)

    def store(h, q):
        return pltpu.make_async_copy(stage.at[q, h % 4], (ko, vo)[q].at[h], osem.at[q, h % 4])

    out(nk - 1).start()
    for q in range(2):
        weights(nk - 1, q).wait()
        for i in range(0, width, 256):
            total = product(nk - 1, q, i)
            for h in (i // HEAD, i // HEAD + 1):
                if h >= 4:
                    store(h - 4, q).wait()
                t = total[:, h * HEAD - i : (h + 1) * HEAD - i]
                stage[q, h % 4] = _turn(t, cos_ref[...], sin_ref[...]) if q == 0 else t.astype(BF16)
                store(h, q).start()
    for q in range(2):
        for h in range(heads - 4, heads):
            store(h, q).wait()
    pltpu.make_async_copy(xv.at[:, :, :depth], xg, xsem).wait()
    for kind in range(7):
        _remote(xv.at[me, :, :depth], xv.at[me, :, :depth], ssem.at[kind], rsem.at[me, 0], mate).wait_send()


def gather(n, x, gain, cos, sin, wk, wv):
    rows, depth = x.shape
    width = wk.shape[1]
    heads, tokens = width // HEAD, n * rows
    nk = depth // KC
    vmem, hbm = pl.BlockSpec(memory_space=pltpu.VMEM), pl.BlockSpec(memory_space=pl.ANY)
    flops = 2 * tokens * depth * width * 2
    return pl.pallas_call(
        functools.partial(_gather, n),
        out_shape=[jax.ShapeDtypeStruct((n, rows, depth), BF16)] + [jax.ShapeDtypeStruct((heads, tokens, HEAD), BF16)] * 2,
        in_specs=[vmem] * 4 + [hbm] * 2,
        out_specs=[hbm] * 3,
        scratch_shapes=[
            pltpu.VMEM((n, rows, depth + PAD), BF16),
            pltpu.VMEM((2, tokens, width + PAD), F32),
            pltpu.VMEM((2, 2, KC, width), BF16),
            pltpu.VMEM((2, 4, tokens, HEAD), BF16),
            pltpu.VMEM((rows, 128), F32),
            pltpu.SemaphoreType.DMA((2, 2)),
            pltpu.SemaphoreType.DMA((7,)),
            pltpu.SemaphoreType.DMA((n, nk)),
            pltpu.SemaphoreType.DMA((2, 4)),
            pltpu.SemaphoreType.DMA,
        ],
        compiler_params=pltpu.CompilerParams(collective_id=0, has_side_effects=True, vmem_limit_bytes=63 * 2**20),
        cost_estimate=pl.CostEstimate(flops=flops, bytes_accessed=2 * (2 * depth * width + 2 * tokens * depth), transcendentals=0),
        name="gather",
    )(x, gain, cos, sin, wk, wv)


NC = 1024
KQ = 1792


def _finish(n, x, cos_ref, sin_ref, kh, vh, xg, wq, wo, y, qacc, qh, seen, xt, wb, term, half, mates, keep, relay, ends, first, second,
            xres, yres, kk, vv, cap, wsem, tsem, hsem, msem, relay_sem, end_sem, send_sem, xsem, ysem, ksem):
    rows, depth = x.shape
    width = wq.shape[1]
    heads = width // HEAD
    nq, nc = depth // KQ, depth // NC
    cuts = [(i, min(NC, width - i)) for i in range(0, width, NC)]
    nu = nq * len(cuts)
    scale = HEAD**-0.5 * LOG2E
    me, mate, right, left, far = _around(n)
    chips = n // 2
    chip, core = lax.div(me, 2), lax.rem(me, 2)
    starts = [sum(SETS[:s]) for s in range(len(SETS))]

    def wq_copy(i, b, slot):
        at, size = cuts[b]
        return pltpu.make_async_copy(wq.at[_ds(i, KQ), at : at + size], wb.at[slot, :, :size], wsem.at[slot])

    def wo_copy(j, slot):
        return pltpu.make_async_copy(wo.at[:, _ds(j, NC)], wb.at[slot, :, :NC], wsem.at[slot])

    q_slot = lambda i, b, s: lax.rem(i * len(cuts) + b + s * (nu + nc), 3)
    o_slot = lambda j, s: lax.rem(j + nu + s * (nu + nc), 3)

    def xt_copy(i, s):
        m = SETS[s]
        return pltpu.make_async_copy(xg.at[:, starts[s] : starts[s] + m, _ds(i, KQ)], xt.at[lax.rem(i, 2), :, :m, :KQ], tsem.at[lax.rem(i, 2)])

    for u in range(2):
        wq_copy(u // len(cuts), u % len(cuts), q_slot(u // len(cuts), u % len(cuts), 0)).start()
    xt_copy(0, 0).start()
    kv_copies = [pltpu.make_async_copy(a, b, ksem.at[i]) for i, (a, b) in enumerate(((kh, kk), (vh, vv)))]
    for c in kv_copies:
        c.start()
    _greet(mate, right, left)

    def to_mate(j, s):
        slot, m = lax.rem(j + s * nc, 4), SETS[s]
        return _remote(half.at[slot, :, :m], mates.at[slot, :, :m], hsem.at[slot], msem.at[slot], mate)

    def sends(j, s):
        m, par, even = SETS[s], s % 2, lax.rem(j, 2) == 0
        cols = _ds(j, NC)
        a = _remote(first.at[0, :m, cols], relay.at[par, :m, cols], send_sem.at[0], relay_sem.at[par, j], jnp.where(even, right, left))
        side = jnp.where(even, 1, 0)
        b = _remote(first.at[1, :m, cols], ends.at[par, side, :m, cols], send_sem.at[1], end_sem.at[par, side, j], jnp.where(even, left, right))
        return a, b

    def last_send(j, s):
        m, par, even = SETS[s], s % 2, lax.rem(j, 2) == 0
        cols = _ds(j, NC)
        side = jnp.where(even, 0, 1)
        return _remote(second.at[:m, cols], ends.at[par, side, :m, cols], send_sem.at[2], end_sem.at[par, side, j], jnp.where(even, right, left))

    def pair_wait(j, s):
        to_mate(j, s).wait_recv()

    def pair_work(j, s):
        slot, m, even = lax.rem(j + s * nc, 4), SETS[s], lax.rem(j, 2) == 0
        cols = _ds(j, NC)
        both = lambda i: term[slot, i, :m] + mates[slot, i, :m].astype(F32)
        near = jnp.where(even, 3, 1)
        keep[0, :m, cols] = both(0)
        keep[1, :m, cols] = both(4 - near)
        first[0, :m, cols] = both(2).astype(BF16)
        first[1, :m, cols] = both(near).astype(BF16)

    def pair_send(j, s):
        for c in sends(j, s):
            c.start()

    def relay_wait(j, s):
        sends(j, s)[0].wait_recv()

    def relay_work(j, s):
        m, cols = SETS[s], _ds(j, NC)
        second[:m, cols] = (keep[1, :m, cols] + relay[s % 2, :m, cols].astype(F32)).astype(BF16)

    def end_wait(j, s):
        sends(j, s)[1].wait_recv()
        last_send(j, s).wait_recv()

    def end_work(j, s):
        m, par, cols = SETS[s], s % 2, _ds(j, NC)
        total = keep[0, :m, cols] + ends[par, 0, :m, cols].astype(F32) + ends[par, 1, :m, cols].astype(F32)
        yres[:m, cols] = (xres[:m, cols].astype(F32) + total).astype(BF16)

    def y_copy(j, s):
        m, cols = SETS[s], _ds(j, NC)
        return pltpu.make_async_copy(yres.at[:m, cols], y.at[starts[s] : starts[s] + m, cols], ysem)

    def x_copy(s):
        m = SETS[s]
        return pltpu.make_async_copy(x.at[starts[s] : starts[s] + m, :], xres.at[:m, :], xsem)

    def sent(s):
        m = SETS[s]
        for kind in range(3):
            _remote(second.at[:m, :], second.at[:m, :], send_sem.at[kind], relay_sem.at[0, 0], mate).wait_send()

    def written(s):
        m = SETS[s]
        pltpu.make_async_copy(yres.at[:m, :], y.at[starts[s] : starts[s] + m, :], ysem).wait()

    def each(lo, hi, work):
        lax.fori_loop(lo, hi, lambda j, c: (work(j), c)[1], 0)

    for s, m in enumerate(SETS):
        size = n * m
        more = s + 1 < len(SETS)

        qacc[:size, :width] = jnp.zeros((size, width), F32)

        def step(i, relayed):
            @pl.when(i + 1 < nq)
            def _():
                xt_copy(i + 1, s).start()

            xt_copy(i, s).wait()
            for b, (at, cut) in enumerate(cuts):
                ahead = b + 2
                i2, b2 = i + ahead // len(cuts), ahead % len(cuts)

                @pl.when(i2 < nq)
                def _():
                    wq_copy(i2, b2, q_slot(i2, b2, s)).start()

                @pl.when(i2 >= nq)
                def _():
                    j2 = (i2 - nq) * len(cuts) + b2
                    wo_copy(j2, o_slot(j2, s)).start()

                slot = q_slot(i, b, s)
                wq_copy(i, b, slot).wait()
                if relayed:
                    relay_wait(i * len(cuts) + b, s - 1)
                    relay_work(i * len(cuts) + b, s - 1)
                states = xt[lax.rem(i, 2), :, :m, :KQ].reshape(size, KQ)
                for o in range(0, cut, 256):
                    qacc[:size, at + o : at + o + 256] += _dot(states, wb[slot, :, o : o + 256])
                if relayed:
                    last_send(i * len(cuts) + b, s - 1).start()

        if s == 0:
            each(0, nq, lambda i: step(i, False))
        else:
            lots = nc // len(cuts)
            each(0, lots, lambda i: step(i, True))
            each(lots, nq, lambda i: step(i, False))
        if more:
            xt_copy(0, s + 1).start()

        cos = cos_ref[:, starts[s] : starts[s] + m, :].reshape(size, HEAD)
        sin = sin_ref[:, starts[s] : starts[s] + m, :].reshape(size, HEAD)

        def turn(h):
            qh[h, :size] = _turn(qacc[:size, _ds(h, HEAD)], cos, sin)

        each(0, heads, turn)

        if s == 0:
            for c in kv_copies:
                c.wait()
        band, keys = 2 * m, 2 * rows
        row, key = (lax.broadcasted_iota(jnp.int32, (band, keys), i) for i in range(2))
        cap[:band] = jnp.where(key <= row + starts[s] + jnp.where(row < m, 0, rows - m), jnp.inf, -jnp.inf)

        def attend(h):
            bands = range(chips)
            cut = lambda a, i, size=band: a[i * size : (i + 1) * size]
            scores = [_dot(qh[h, b * band : size], kk[h, b * keys : (b + 1) * keys], 1, 1) for b in bands]
            weights = []
            for g in bands:
                mine = [cut(scores[b], g - b) for b in range(g + 1)]
                mine[g] = jnp.minimum(mine[g], cap[:band])
                top = functools.reduce(jnp.maximum, mine).max(axis=1, keepdims=True)
                weights.append([jnp.exp2((score - top) * scale).astype(BF16) for score in mine])
            ones = jnp.ones((keys, HEAD), BF16)
            mixes = []
            for b in bands:
                values = jnp.concatenate([vv[h, b * keys : (b + 1) * keys], ones], axis=1)
                mixes.append(_dot(jnp.concatenate([weights[g][b] for g in range(b, chips)], axis=0), values))
            for g in bands:
                mix = sum(cut(mixes[b], g - b) for b in range(g + 1))
                found = (mix[:, :HEAD] / mix[:, HEAD:]).astype(BF16)
                for i in range(2):
                    to = lax.rem(g - chip + chips, chips) + jnp.where(core == i, 0, chips)
                    seen[to, :m, _ds(h, HEAD)] = cut(found, i, m)

        lax.fori_loop(0, heads, lambda h, c: (attend(h), c)[1], 0, unroll=2)

        if s > 0:
            sent(s - 1)
            x_copy(s - 1).wait()

        def project(j, paired, ended):
            @pl.when(j + 2 < nc)
            def _():
                wo_copy(j + 2, o_slot(j + 2, s)).start()

            if more:
                @pl.when(j + 2 >= nc)
                def _():
                    u = j + 2 - nc
                    for b in range(len(cuts)):
                        @pl.when(u == b)
                        def _():
                            wq_copy(0, b, q_slot(0, b, s + 1)).start()

            slot = o_slot(j, s)
            if paired:
                pair_wait(j - 2, s)

            @pl.when(j >= 4)
            def _():
                to_mate(j - 4, s).wait_send()

            if ended:
                end_wait(j, s - 1)
            wo_copy(j, slot).wait()
            if paired:
                pair_work(j - 2, s)
            if ended:
                end_work(j, s - 1)
            states = seen[:, :m, :width].reshape(size, width)
            ring = lax.rem(j + s * nc, 4)
            for o in range(0, NC, 256):
                got = _dot(states, wb[slot, :, o : o + 256]).reshape(n, m, 256)
                term[ring, :, :m, o : o + 256] = got[:chips]
                half[ring, :, :m, o : o + 256] = got[chips:].astype(BF16)
            to_mate(j, s).start()
            if paired:
                pair_send(j - 2, s)
            if ended:
                y_copy(j, s - 1).start()

        each(0, 2, lambda j: project(j, False, s > 0))
        each(2, nc, lambda j: project(j, True, s > 0))
        for j in (nc - 2, nc - 1):
            pair_wait(j, s)
            pair_work(j, s)
            pair_send(j, s)
        for j in range(nc - 4, nc):
            to_mate(j, s).wait_send()
        if s > 0:
            written(s - 1)
        x_copy(s).start()

    last = len(SETS) - 1
    x_copy(last).wait()

    def relay_all(j):
        relay_wait(j, last)
        relay_work(j, last)
        last_send(j, last).start()

    def end_all(j):
        end_wait(j, last)
        end_work(j, last)
        y_copy(j, last).start()

    each(0, nc, relay_all)
    each(0, nc, end_all)
    sent(last)
    written(last)


def finish(n, x, cos, sin, kk, vv, xg, wq, wo):
    rows, depth = x.shape
    width = wq.shape[1]
    heads, tokens = width // HEAD, n * rows
    nc, chips, m = depth // NC, n // 2, max(SETS)
    vmem, hbm = pl.BlockSpec(memory_space=pltpu.VMEM), pl.BlockSpec(memory_space=pl.ANY)
    flops = 2 * tokens * depth * width * 2
    dma = pltpu.SemaphoreType.DMA
    return pl.pallas_call(
        functools.partial(_finish, n),
        out_shape=jax.ShapeDtypeStruct((rows, depth), BF16),
        in_specs=[hbm, vmem, vmem, hbm, hbm, hbm, hbm, hbm],
        out_specs=hbm,
        scratch_shapes=[
            pltpu.VMEM((n * m, width + PAD), F32),
            pltpu.VMEM((heads, n * m, HEAD), BF16),
            pltpu.VMEM((n, m, width + PAD), BF16),
            pltpu.VMEM((2, n, m, KQ + PAD), BF16),
            pltpu.VMEM((3, KQ, NC + PAD), BF16),
            pltpu.VMEM((4, chips, m, NC), F32),
            pltpu.VMEM((4, chips, m, NC), BF16),
            pltpu.VMEM((4, chips, m, NC), BF16),
            pltpu.VMEM((2, m, depth), F32),
            pltpu.VMEM((2, m, depth), BF16),
            pltpu.VMEM((2, 2, m, depth), BF16),
            pltpu.VMEM((2, m, depth), BF16),
            pltpu.VMEM((m, depth), BF16),
            pltpu.VMEM((m, depth), BF16),
            pltpu.VMEM((m, depth), BF16),
            pltpu.VMEM((heads, tokens, HEAD), BF16),
            pltpu.VMEM((heads, tokens, HEAD), BF16),
            pltpu.VMEM((2 * m, 2 * rows), F32),
            dma((3,)), dma((2,)), dma((4,)), dma((4,)), dma((2, nc)), dma((2, 2, nc)), dma((3,)), dma, dma, dma((2,)),
        ],
        compiler_params=pltpu.CompilerParams(collective_id=1, has_side_effects=True, vmem_limit_bytes=63 * 2**20),
        cost_estimate=pl.CostEstimate(flops=flops, bytes_accessed=2 * 2 * 3 * depth * width, transcendentals=0),
        name="finish",
    )(x, cos, sin, kk, vv, xg, wq, wo)


def solution(mesh):
    n = mesh.shape["tp"]

    def step(x, gain, wq, wk, wv, wo):
        rows = x.shape[0]
        half = HEAD // 2
        angle = np.arange(n * rows)[:, None] * float(THETA) ** (-np.arange(half) / half)
        cos = np.concatenate([np.cos(angle), np.cos(angle)], 1).astype(np.float32)
        sin = np.concatenate([-np.sin(angle), np.sin(angle)], 1).astype(np.float32)
        xg, kk, vv = gather(n, x, gain[None], jnp.asarray(cos), jnp.asarray(sin), wk, wv)
        shape = (n, rows, HEAD)
        return finish(n, x, jnp.asarray(cos).reshape(shape), jnp.asarray(sin).reshape(shape), kk, vv, xg, wq, wo)

    tokens, columns = P(("dp", "tp"), None), P(None, "tp")
    return jax.shard_map(
        step,
        mesh=mesh,
        in_specs=(tokens, P(None), columns, columns, columns, P("tp", None)),
        out_specs=tokens,
        check_vma=False,
    )
```
